32 devices in a mesh: seq: 8 (over z, y), tp: 4 (over x, core).
Axes of the slice: x: 2, y: 2, z: 4, core: 2. Of those that a mesh axis runs over, the one named last changes fastest.
Arguments:
- mixer_input: bfloat16 [1024, 8192], P('seq', 'tp'), may hold values from -6 to 6
- gate_input: bfloat16 [1024, 8192], P('seq', 'tp'), may hold values from -6 to 6
- input_matrix: bfloat16 [1024, 1024], P('seq', 'tp'), may hold values from -6 to 6
- output_matrix: bfloat16 [1024, 1024], P('seq', 'tp'), may hold values from -6 to 6
- step_raw: float32 [1024, 128], P('seq', 'tp'), may hold values from -3 to 3
- step_bias: float32 [128], P('tp'), may hold values from -1 to 0.5
- decay_rate: float32 [128], P('tp'), may hold values from 0.0001 to 0.05
- skip_weight: float32 [128], P('tp'), may hold values from 0.5 to 1.5
- conv_mixer: float32 [4, 8192], P(None, 'tp'), may hold values from -3 to 3
- conv_input: float32 [4, 1024], P(None, 'tp'), may hold values from -3 to 3
- conv_output: float32 [4, 1024], P(None, 'tp'), may hold values from -3 to 3
- norm_gain: float32 [8192], P('tp'), may hold values from 0.5 to 1.5
- queries: bfloat16 [1024, 8192], P('seq', 'tp'), may hold values from -5 to 5
- keys: bfloat16 [1024, 1024], P('seq', 'tp'), may hold values from -5 to 5
- values: bfloat16 [1024, 1024], P('seq', 'tp'), may hold values from -6 to 6
Outputs:
- mixer_out: bfloat16 [1024, 8192], P('seq', 'tp')
- attention_out: bfloat16 [1024, 8192], P('seq', 'tp')
The draws below stay inside these ranges and needn't reach their ends.
All inputs are finite; a program needn't handle non-finite values.
Results may differ from the reference program's by a relative error of at most 0.007.
Values may be sent and summed in bfloat16 or wider, within the bound.
A program may use at most 192 MiB of HBM per device.

```python
import math
import jax
import jax.numpy as jnp
from jax import lax

MH = 128
P_SIZE = 64
STATE = 128
GROUPS = 8
QH = 64
KVH = 8
HD = 128
CONV = 4
SCAN_BLOCK = 128
INNER = 8192
TOKENS = 1024


def draw_queries(key, part):
    drawn = jnp.clip(jax.random.normal(jax.random.fold_in(key, 1), (TOKENS, QH * HD), jnp.float32), -5.0, 5.0)
    return drawn.astype(jnp.bfloat16)


def draw_keys(key, part):
    drawn = jnp.clip(jax.random.normal(jax.random.fold_in(key, 2), (TOKENS, KVH * HD), jnp.float32), -5.0, 5.0)
    return drawn.astype(jnp.bfloat16)


def block_levels(stream_key, shape, cuts, least, top_value):
    factor_of = 1.0
    for dim, parts in cuts:
        draws = jax.random.uniform(jax.random.fold_in(jax.random.fold_in(stream_key, 6), dim), (parts,), jnp.float32, least / len(cuts), top_value / len(cuts))
        factor_of = factor_of * jnp.repeat(jnp.exp(draws), shape[dim] // parts).reshape((-1,) + (1,) * (len(shape) - 1 - dim))
    return factor_of


def normal_values(own_key, extent, width, bound, shards=(), held_as=jnp.bfloat16):
    values = width * jax.random.normal(own_key, extent, jnp.float32)
    if shards:
        values = values * block_levels(own_key, extent, shards, -0.22, 0.18)
    return jnp.clip(values, -bound, bound).astype(held_as)


def setup_inputs(seed: int = 0) -> dict:
    splits = jax.random.split(jax.random.key(seed), 16)
    mixer_input = normal_values(splits[0], (TOKENS, INNER), 1.0, 6.0, ((0, 8), (1, 4)))
    gate_input = normal_values(splits[1], (TOKENS, INNER), 1.0, 6.0, ((0, 8), (1, 4)))
    input_matrix = normal_values(splits[2], (TOKENS, GROUPS * STATE), 1.0, 6.0, ((0, 8), (1, 4)))
    output_matrix = normal_values(splits[3], (TOKENS, GROUPS * STATE), 1.0, 6.0, ((0, 8), (1, 4)))
    step_raw = normal_values(splits[4], (TOKENS, MH), 0.5, 3.0, ((0, 8), (1, 4)), jnp.float32)
    step_bias = jnp.clip(-1.0 + 1.5 * jax.random.uniform(splits[5], (MH,), jnp.float32) ** block_levels(splits[5], (MH,), ((0, 4),), -0.2, 0.2), -1.0, 0.5)
    decay_rate = jnp.clip(jnp.exp(math.log(0.05) - 6.214608 * jax.random.uniform(splits[6], (MH,), jnp.float32) ** block_levels(splits[6], (MH,), ((0, 4),), -0.2, 0.2)), 0.0001, 0.05)
    skip_weight = jnp.clip(0.5 + 1.0 * jax.random.uniform(splits[7], (MH,), jnp.float32) ** block_levels(splits[7], (MH,), ((0, 4),), -0.2, 0.2), 0.5, 1.5)
    conv_mixer = normal_values(splits[8], (CONV, INNER), CONV ** -0.5, 3.0, ((1, 4),), jnp.float32)
    conv_input = normal_values(splits[9], (CONV, GROUPS * STATE), CONV ** -0.5, 3.0, ((1, 4),), jnp.float32)
    conv_output = normal_values(splits[10], (CONV, GROUPS * STATE), CONV ** -0.5, 3.0, ((1, 4),), jnp.float32)
    norm_gain = jnp.clip(1.0 + 0.1 * jax.random.normal(splits[11], (INNER,), jnp.float32), 0.5, 1.5)
    queries = draw_queries(jax.random.fold_in(splits[15], 71), 0)
    keys = draw_keys(jax.random.fold_in(splits[15], 71), 0)
    values = normal_values(splits[14], (TOKENS, KVH * HD), 1.0, 6.0, ((0, 8), (1, 4)))
    return {"mixer_input": mixer_input, "gate_input": gate_input, "input_matrix": input_matrix, "output_matrix": output_matrix, "step_raw": step_raw, "step_bias": step_bias, "decay_rate": decay_rate, "skip_weight": skip_weight, "conv_mixer": conv_mixer, "conv_input": conv_input, "conv_output": conv_output, "norm_gain": norm_gain, "queries": queries, "keys": keys, "values": values}


HIGHEST = lax.Precision.HIGHEST
norm_epsilon = 1e-05
lowest_score = -1e+30

def conv_silu(raw_rows, weights, history):
    padded = jnp.concatenate([history, raw_rows], axis=0).astype(jnp.float32)
    length = raw_rows.shape[0]
    summed = jnp.zeros((length, raw_rows.shape[1]), jnp.float32)
    for offset in range(weights.shape[0]):
        summed = summed + weights[offset][None, :] * padded[offset:offset + length]
    return jax.nn.silu(summed)

def ssd_block(signal, b_state, c_state, step_size, rates, carried):
    group_heads = signal.shape[1] // b_state.shape[1]
    log_decay = jnp.cumsum(-step_size * rates[None, :], axis=0)
    length = signal.shape[0]
    places = jnp.arange(length, dtype=jnp.int32)
    causal = (places[:, None] >= places[None, :])[:, :, None]
    spread = jnp.where(causal, log_decay[:, None, :] - log_decay[None, :, :], 0.0)
    decays = jnp.where(causal, jnp.exp(spread), 0.0)
    coupling = jnp.einsum('tgn,sgn->gts', c_state, b_state, precision=HIGHEST)
    coupling = jnp.repeat(coupling, group_heads, axis=0)
    mixing = jnp.transpose(decays, (2, 0, 1)) * coupling
    scaled = signal * step_size[:, :, None]
    output = jnp.einsum('hts,shp->thp', mixing, scaled, precision=HIGHEST)
    b_heads = jnp.repeat(b_state, group_heads, axis=1)
    c_heads = jnp.repeat(c_state, group_heads, axis=1)
    output = output + jnp.exp(log_decay)[:, :, None] * jnp.einsum('thn,hpn->thp', c_heads, carried, precision=HIGHEST)
    closing = jnp.exp(log_decay[-1][None, :] - log_decay)
    weighted = scaled * closing[:, :, None]
    updated = jnp.exp(log_decay[-1])[:, None, None] * carried + jnp.einsum('shp,shn->hpn', weighted, b_heads, precision=HIGHEST)
    return (output, updated, log_decay, c_heads)

def attend_update(carry, query_block, query_start, key_block, value_block, key_start, widen):
    maxima, totals, accum = carry
    kv_heads = key_block.shape[1] // HD
    grouped = query_block.shape[1] // HD // kv_heads
    query_rows = query_block.shape[0]
    key_rows = key_block.shape[0]
    query_four = query_block.reshape(query_rows, kv_heads, grouped, HD)
    key_three = key_block.reshape(key_rows, kv_heads, HD)
    value_three = value_block.reshape(key_rows, kv_heads, HD)
    if widen:
        scores = jnp.einsum('qhgd,khd->hgqk', query_four.astype(jnp.float32), key_three.astype(jnp.float32))
    else:
        scores = jnp.einsum('qhgd,khd->hgqk', query_four, key_three, preferred_element_type=jnp.float32)
    scores = scores * (1.0 / math.sqrt(HD))
    query_places = query_start + jnp.arange(query_rows, dtype=jnp.int32)
    key_places = key_start + jnp.arange(key_rows, dtype=jnp.int32)
    allowed = key_places[None, :] <= query_places[:, None]
    masked = jnp.where(allowed, scores, lowest_score)
    newmax = jnp.maximum(maxima, lax.optimization_barrier(jnp.max(masked, axis=-1)))
    probs = jnp.where(allowed, jnp.exp(masked - newmax[..., None]), 0.0)
    factor = jnp.exp(maxima - newmax)
    totals = totals * factor + lax.optimization_barrier(jnp.sum(probs, axis=-1))
    rounded = probs.astype(jnp.bfloat16)
    if widen:
        product = jnp.einsum('hgqk,khd->hgqd', rounded.astype(jnp.float32), value_three.astype(jnp.float32))
    else:
        product = jnp.einsum('hgqk,khd->hgqd', rounded, value_three, preferred_element_type=jnp.float32)
    accum = accum * factor[..., None] + product
    return (newmax, totals, accum)

def finish(carry):
    maxima, totals, accum = carry
    result = accum / totals[..., None]
    result = jnp.transpose(result, (2, 0, 1, 3))
    return result.reshape(result.shape[0], -1).astype(jnp.bfloat16)

def attention(queries, keys, values):
    span = math.gcd(TOKENS, 512)
    count = TOKENS // span
    grouped = QH // KVH

    def one_block(index):
        start = index * span
        query_block = lax.dynamic_slice_in_dim(queries, start, span, 0)
        initial = (jnp.full((KVH, grouped, span), lowest_score, jnp.float32), jnp.zeros((KVH, grouped, span), jnp.float32), jnp.zeros((KVH, grouped, span, HD), jnp.float32))

        def visit(position, carry):
            key_start = position * span
            key_block = lax.dynamic_slice_in_dim(keys, key_start, span, 0)
            value_block = lax.dynamic_slice_in_dim(values, key_start, span, 0)
            return attend_update(carry, query_block, start, key_block, value_block, key_start, True)
        return finish(lax.fori_loop(0, index + 1, visit, initial))
    blocks = lax.map(one_block, jnp.arange(count, dtype=jnp.int32))
    return blocks.reshape(TOKENS, QH * HD)

def reference(mixer_input, gate_input, input_matrix, output_matrix, step_raw, step_bias, decay_rate, skip_weight, conv_mixer, conv_input, conv_output, norm_gain, queries, keys, values):
    reach = CONV - 1
    signal = conv_silu(mixer_input, conv_mixer, jnp.zeros((reach, mixer_input.shape[1]), jnp.bfloat16))
    b_state = conv_silu(input_matrix, conv_input, jnp.zeros((reach, input_matrix.shape[1]), jnp.bfloat16))
    c_state = conv_silu(output_matrix, conv_output, jnp.zeros((reach, output_matrix.shape[1]), jnp.bfloat16))
    signal = signal.reshape(TOKENS, MH, P_SIZE)
    b_state = b_state.reshape(TOKENS, GROUPS, STATE)
    c_state = c_state.reshape(TOKENS, GROUPS, STATE)
    step_size = jax.nn.softplus(step_raw + step_bias[None, :])
    blocks = TOKENS // SCAN_BLOCK

    def advance(carried, pieces):
        signal_part, b_part, c_part, step_part = pieces
        output, updated, log_decay, c_heads = ssd_block(signal_part, b_part, c_part, step_part, decay_rate, carried)
        return (updated, output)
    _, outputs = lax.scan(advance, jnp.zeros((MH, P_SIZE, STATE), jnp.float32), (signal.reshape(blocks, SCAN_BLOCK, MH, P_SIZE), b_state.reshape(blocks, SCAN_BLOCK, GROUPS, STATE), c_state.reshape(blocks, SCAN_BLOCK, GROUPS, STATE), step_size.reshape(blocks, SCAN_BLOCK, MH)))
    mixed = outputs.reshape(TOKENS, MH, P_SIZE) + skip_weight[None, :, None] * signal
    gated = mixed.reshape(TOKENS, MH * P_SIZE) * jax.nn.silu(gate_input.astype(jnp.float32))
    squares = lax.optimization_barrier(jnp.mean(gated * gated, axis=1, keepdims=True))
    mixer_out = (gated * lax.rsqrt(squares + norm_epsilon) * norm_gain[None, :]).astype(jnp.bfloat16)
    attention_out = attention(queries, keys, values)
    return (mixer_out, attention_out)
```

```python
import functools
import math

import jax
import jax.numpy as jnp
from jax import lax
from jax.experimental import pallas as pl
from jax.experimental.pallas import tpu as pltpu
from jax.sharding import PartitionSpec as P


P_SIZE = 64
STATE = 128
HD = 128
COLS = 2
CHUNKS = 4
HALO = 16
EPS = 1e-05
LOWEST = -1e30
MESH = pl.DeviceIdType.MESH
F32 = jnp.float32
BF16 = jnp.bfloat16


def dot(a, b, ca=1, cb=0):
    return lax.dot_general(a, b, (((ca,), (cb,)), ((), ())), preferred_element_type=F32)


def pieces_of(a, terms):
    out = []
    for _ in range(terms):
        head = a.astype(BF16)
        out.append(head)
        a = a - head.astype(F32)
    return out


def silu(a):
    return a / (1.0 + jnp.exp(-a))


def kernel(
    n, tp, inner,
    x_ref, gate_ref, b_ref, c_ref, step_ref, bias_ref, rate_ref, skip_ref,
    cx_ref, cb_ref, cc_ref, gain_ref, q_ref, k_ref, v_ref,
    mix_out, att_out,
    hx, hb, hc, padx, padb, sig, wgt, scl, ex, bst, cst,
    s_buf, r1, e_in, e_out, p_out, ent, p_in, dec_own, dec_par,
    kbuf, vbuf, qs, acc, m_sc, l_sc, ybuf, sq_own, sq_in,
    halo_s, halo_r, dec_s, dec_r, p1_s, p1_r, p2_s, p2_r, p3_s, p3_r,
    kc_s, kc_r, kp_s, kp_r, kl_s, sq_s, sq_r,
):
    me = lax.axis_index("seq")
    mytp = lax.axis_index("tp")
    rows = n // COLS
    row = me // COLS
    col = me % COLS
    other = 1 - col
    partner = row * COLS + other
    length, width = x_ref.shape
    half = width // 2
    cw = half // CHUNKS
    groups = b_ref.shape[1] // STATE
    gwidth = width // groups
    heads = width // P_SIZE
    kvh = k_ref.shape[1] // HD
    qper = q_ref.shape[1] // HD // kvh

    barrier = pltpu.get_barrier_semaphore()

    @pl.loop(1, n)
    def _(d):
        pl.semaphore_signal(barrier, inc=1, device_id={"seq": (me + d) % n}, device_id_type=MESH)

    for d in range(1, tp):
        pl.semaphore_signal(
            barrier, inc=1, device_id={"tp": (mytp + d) % tp}, device_id_type=MESH
        )

    pre = step_ref[...] + bias_ref[...]
    dt = jnp.maximum(pre, 0.0) + jnp.log1p(jnp.exp(-jnp.abs(pre)))
    a = -dt * rate_ref[...]
    ri = lax.broadcasted_iota(jnp.int32, (length, length), 0)
    ci = lax.broadcasted_iota(jnp.int32, (length, length), 1)
    lower = (ri >= ci).astype(F32).astype(BF16)
    upper = (ri <= ci).astype(F32).astype(BF16)
    apieces = pieces_of(a, 3)
    logd = sum(dot(lower, p) for p in apieces)
    logt = sum(dot(p, upper, 0, 0) for p in apieces)
    last = logd[length - 1 : length, :]
    closing = jnp.exp(last - logd)
    hi = lax.broadcasted_iota(jnp.int32, (heads, width), 0)
    wi = lax.broadcasted_iota(jnp.int32, (heads, width), 1)
    spread = (wi // P_SIZE == hi).astype(F32).astype(BF16)
    many = jnp.concatenate([dt, dt * closing, jnp.exp(logd)], axis=0)
    wide = sum(dot(p, spread) for p in pieces_of(many, 2))
    dtx, wx, elx = wide[:length], wide[length : 2 * length], wide[2 * length :]
    skipx = sum(dot(p, spread) for p in pieces_of(jnp.broadcast_to(skip_ref[...], (8, heads)), 3))[:1]
    for h in range(2):
        cut = slice(h * half, (h + 1) * half)
        ex[h] = elx[:, cut]
        scl[h] = dtx[:, cut]
        sig[h] = wx[:, cut]
        dec_own[h] = elx[length - 1 : length, cut]

    pl.semaphore_wait(barrier, n - 1 + tp - 1)

    def halo(dst):
        out = []
        for i, (src, buf) in enumerate(((x_ref, hx), (b_ref, hb), (c_ref, hc))):
            out.append(
                pltpu.make_async_remote_copy(
                    src_ref=src.at[pl.ds(length - HALO, HALO)], dst_ref=buf,
                    send_sem=halo_s.at[i], recv_sem=halo_r.at[i],
                    device_id={"seq": dst}, device_id_type=MESH,
                )
            )
        return out

    @pl.when(me < n - 1)
    def _():
        for cp in halo(me + 1):
            cp.start()

    dec_copy = pltpu.make_async_remote_copy(
        src_ref=dec_own, dst_ref=dec_par, send_sem=dec_s.at[0], recv_sem=dec_r.at[0],
        device_id={"seq": partner}, device_id_type=MESH,
    )
    dec_copy.start()

    def place(c):
        return pl.ds(pl.multiple_of(c * length, length), length)

    def kv_copy(i, dst_row, dst_col, slot_row, slot_col, own, ss, rs, sidx, ridx):
        src = (k_ref, v_ref)[i] if own else (kbuf, vbuf)[i].at[slot_row, place(slot_col)]
        return pltpu.make_async_remote_copy(
            src_ref=src, dst_ref=(kbuf, vbuf)[i].at[slot_row, place(slot_col)],
            send_sem=ss.at[i, sidx], recv_sem=rs.at[i, ridx],
            device_id={"seq": dst_row * COLS + dst_col}, device_id_type=MESH,
        )

    def own_up(i, dst_row):
        return kv_copy(i, dst_row, col, row, col, True, kc_s, kc_r, dst_row, row)

    def own_side(i):
        return kv_copy(i, row, other, row, col, True, kl_s, kp_r, 0, row)

    def relay(i, src_row):
        return kv_copy(i, row, other, src_row, col, False, kp_s, kp_r, src_row, src_row)

    @pl.loop(row + 1, rows)
    def _(dst):
        for i in range(2):
            own_up(i, dst).start()

    for i in range(2):
        own_side(i).start()

    kbuf[row, place(col)] = k_ref[...]
    vbuf[row, place(col)] = v_ref[...]
    for g in range(kvh):
        for h in range(qper):
            at = (g * qper + h) * HD
            qs[g, h * length : (h + 1) * length] = q_ref[:, at : at + HD]

    @pl.when(me > 0)
    def _():
        for cp in halo(me):
            cp.wait_recv()
        padx[:HALO] = hx[...].astype(F32)
        padb[0, :HALO] = hb[...].astype(F32)
        padb[1, :HALO] = hc[...].astype(F32)

    @pl.when(me == 0)
    def _():
        padx[:HALO] = jnp.zeros((HALO, width), F32)
        padb[:, :HALO] = jnp.zeros((2, HALO, b_ref.shape[1]), F32)

    padx[HALO:] = x_ref[...].astype(F32)
    padb[0, HALO:] = b_ref[...].astype(F32)
    padb[1, HALO:] = c_ref[...].astype(F32)
    taps = cx_ref.shape[0]

    def conv(load, w_ref, cut):
        total = None
        for k in range(taps):
            at = HALO - (taps - 1) + k
            term = w_ref[k : k + 1, cut] * load(at)
            total = term if total is None else total + term
        return silu(total)

    for g in range(groups):
        cut = slice(g * STATE, (g + 1) * STATE)
        bst[g] = conv(lambda at: padb[0, at : at + length, cut], cb_ref, cut).astype(BF16)
        cst[g] = conv(lambda at: padb[1, at : at + length, cut], cc_ref, cut).astype(BF16)
    for h in range(2):
        for j in range(CHUNKS):
            cut = slice(h * half + j * cw, h * half + (j + 1) * cw)
            loc = slice(j * cw, (j + 1) * cw)
            s = conv(lambda at: padx[at : at + length, cut], cx_ref, cut)
            wgt[h, j] = (s * sig[h, :, loc]).astype(BF16)
            sig[h, :, loc] = s
            scl[h, :, loc] = s * scl[h, :, loc]

    def group_of(h, j):
        return h * (groups // 2) + (j * cw) // gwidth

    def p1(j):
        return pltpu.make_async_remote_copy(
            src_ref=s_buf.at[other, j], dst_ref=r1.at[j],
            send_sem=p1_s.at[j], recv_sem=p1_r.at[j],
            device_id={"seq": partner}, device_id_type=MESH,
        )

    for j in range(CHUNKS):
        s_buf[other, j] = dot(bst[group_of(other, j)], wgt[other, j], 0, 0).astype(BF16)
        p1(j).start()
    for j in range(CHUNKS):
        s_buf[col, j] = dot(bst[group_of(col, j)], wgt[col, j], 0, 0).astype(BF16)

    @pl.loop(0, row)
    def _(src):
        for i in range(2):
            own = kv_copy(i, row, col, src, col, False, kc_s, kc_r, row, src)
            own.wait_recv()
            relay(i, src).start()

    causal = ri >= ci
    lane = lax.broadcasted_iota(jnp.int32, (length, 128), 1)
    per = 128 // P_SIZE
    for g in range(groups):
        coup = dot(cst[g], bst[g], 1, 1)
        coup = jnp.where(causal, coup, 0.0)
        for t in range(gwidth // 128):
            at = g * gwidth + t * 128
            h, loc = at // half, at % half
            tile = scl[h, :, loc : loc + 128].astype(BF16)
            res = None
            for p in range(per):
                hd = at // P_SIZE + p
                diff = logd[:, hd : hd + 1] - logt[hd : hd + 1, :]
                mixing = (jnp.exp(jnp.minimum(diff, 0.0)) * coup).astype(BF16)
                y = dot(mixing, tile)
                res = y if res is None else jnp.where(lane >= p * P_SIZE, y, res)
            ybuf[h, :, loc : loc + 128] = res + skipx[:, at : at + 128] * sig[h, :, loc : loc + 128]

    scale = math.log2(math.e) / math.sqrt(HD)
    qrows = qper * length

    def attend(lo, hi):
        @pl.loop(lo, hi)
        def _(g):
            m_sc[...] = jnp.full((qrows, 1), LOWEST, F32)
            l_sc[...] = jnp.zeros((qrows, 1), F32)
            acc[...] = jnp.zeros((qrows, HD), F32)
            lanes = pl.ds(pl.multiple_of(g * HD, HD), HD)

            def step(r, masked):
                s = dot(qs[g], kbuf[r, :, lanes], 1, 1) * scale
                if masked:
                    qi = lax.broadcasted_iota(jnp.int32, s.shape, 0) % length + col * length
                    ki = lax.broadcasted_iota(jnp.int32, s.shape, 1)
                    s = jnp.where(ki <= qi, s, LOWEST)
                old = m_sc[...]
                new = jnp.maximum(old, jnp.max(s, axis=1, keepdims=True))
                p = jnp.exp2(s - new)
                f = jnp.exp2(old - new)
                m_sc[...] = new
                l_sc[...] = l_sc[...] * f + jnp.sum(p, axis=1, keepdims=True)
                acc[...] = acc[...] * f + dot(p.astype(BF16), vbuf[r, :, lanes])

            step(row, True)

            @pl.loop(0, row)
            def _(r):
                step(r, False)

            out = (acc[...] / l_sc[...]).astype(BF16)
            for h in range(qper):
                at = pl.multiple_of((g * qper + h) * HD, HD)
                att_out[:, pl.ds(at, HD)] = out[h * length : (h + 1) * length]

    @pl.loop(0, row)
    def _(src):
        for i in range(2):
            relay(i, src).wait_recv()

    for i in range(2):
        own_side(i).wait_recv()
    early = jnp.where(row == rows - 1, kvh, 0)
    attend(0, early)

    dec_copy.wait_recv()

    def p2(j, dst_row):
        return pltpu.make_async_remote_copy(
            src_ref=e_out.at[j], dst_ref=e_in.at[j],
            send_sem=p2_s.at[j], recv_sem=p2_r.at[j],
            device_id={"seq": dst_row * COLS + col}, device_id_type=MESH,
        )

    def p3(j):
        return pltpu.make_async_remote_copy(
            src_ref=p_out.at[j], dst_ref=p_in.at[j],
            send_sem=p3_s.at[j], recv_sem=p3_r.at[j],
            device_id={"seq": partner}, device_id_type=MESH,
        )

    @pl.when(row == 0)
    def _():
        e_in[...] = jnp.zeros(e_in.shape, BF16)

    first_col = col == 0
    for j in range(CHUNKS):
        loc = slice(j * cw, (j + 1) * cw)
        do, dp = dec_own[col, :, loc], dec_par[col, :, loc]
        p1(j).wait_recv()

        @pl.when(row > 0)
        def _():
            p2(j, row).wait_recv()

        so = s_buf[col, j].astype(F32)
        sr = r1[j].astype(F32)
        e = e_in[j].astype(F32)
        earlier = jnp.where(first_col, so, sr)
        later = jnp.where(first_col, sr, so)
        dec_a = jnp.where(first_col, do, dp)
        dec_b = jnp.where(first_col, dp, do)
        mid = dec_a * e + earlier

        @pl.when(row < rows - 1)
        def _():
            e_out[j] = (dec_b * mid + later).astype(BF16)
            p2(j, row + 1).start()

        p_out[j] = jnp.where(first_col, mid, e).astype(BF16)
        p3(j).start()
        ent[j] = jnp.where(first_col, e, mid).astype(BF16)

    attend(early, kvh)

    ones = jnp.ones((8, cw), F32).astype(BF16)
    sums = jnp.zeros((8, length), F32)

    def close(h, j, state):
        loc = slice(j * cw, (j + 1) * cw)
        y = ybuf[h, :, loc] + ex[h, :, loc] * dot(cst[group_of(h, j)], state)
        at = pl.ds(pl.multiple_of(h * half + j * cw, cw), cw)
        y = y * silu(gate_ref[:, at].astype(F32))
        ybuf[h, :, loc] = y
        return y * y

    squares = None
    for j in range(CHUNKS):
        s = close(col, j, ent[j])
        squares = s if squares is None else squares + s
    for j in range(CHUNKS):
        p3(j).wait_recv()
        squares = squares + close(other, j, p_in[j])
    for p in pieces_of(squares, 3):
        sums = sums + dot(ones, p, 1, 1)
    sq_own[...] = sums

    def sq(d):
        return pltpu.make_async_remote_copy(
            src_ref=sq_own, dst_ref=sq_in.at[d - 1],
            send_sem=sq_s.at[d - 1], recv_sem=sq_r.at[d - 1],
            device_id={"tp": (mytp + d) % tp}, device_id_type=MESH,
        )

    for d in range(1, tp):
        sq(d).start()
    for d in range(1, tp):
        sq(d).wait_recv()
        sums = sums + sq_in[d - 1]
    scal = lax.rsqrt(sums / inner + EPS)
    eighth = jnp.full((8, 128), 0.125, F32).astype(BF16)
    column = sum(dot(p, eighth, 0, 0) for p in pieces_of(scal, 3))
    for t in range(width // 128):
        h, loc = (t * 128) // half, (t * 128) % half
        cut = slice(t * 128, (t + 1) * 128)
        mix_out[:, cut] = (ybuf[h, :, loc : loc + 128] * column * gain_ref[:, cut]).astype(BF16)

    for d in range(1, tp):
        sq(d).wait_send()
    for j in range(CHUNKS):
        p1(j).wait_send()
        p3(j).wait_send()
    dec_copy.wait_send()
    for i in range(2):
        own_side(i).wait_send()

    @pl.when(row < rows - 1)
    def _():
        for j in range(CHUNKS):
            p2(j, row + 1).wait_send()

    @pl.when(me < n - 1)
    def _():
        for cp in halo(me + 1):
            cp.wait_send()

    @pl.loop(row + 1, rows)
    def _(dst):
        for i in range(2):
            own_up(i, dst).wait_send()

    @pl.loop(0, row)
    def _(src):
        for i in range(2):
            relay(i, src).wait_send()


def shards(inner, n, tp, x, gate, b, c, step, bias, rate, skip, cx, cb, cc, gain, q, k, v):
    length, width = x.shape
    half = width // 2
    cw = half // CHUNKS
    groups = b.shape[1] // STATE
    kvw = k.shape[1]
    kvh = kvw // HD
    qrows = q.shape[1] // HD // kvh * length
    rows = n // COLS
    vm, dma = pltpu.VMEM, pltpu.SemaphoreType.DMA
    chunk = (CHUNKS, STATE, cw)
    scratch = [
        vm((HALO, width), BF16), vm((HALO, b.shape[1]), BF16), vm((HALO, b.shape[1]), BF16),
        vm((HALO + length, width), F32), vm((2, HALO + length, b.shape[1]), F32),
        vm((2, length, half), F32), vm((2, CHUNKS, length, cw), BF16),
        vm((2, length, half), F32), vm((2, length, half), F32),
        vm((groups, length, STATE), BF16), vm((groups, length, STATE), BF16),
        vm((2,) + chunk, BF16), vm(chunk, BF16), vm(chunk, BF16), vm(chunk, BF16),
        vm(chunk, BF16), vm(chunk, BF16), vm(chunk, BF16),
        vm((2, 1, half), F32), vm((2, 1, half), F32),
        vm((rows, COLS * length, kvw), BF16), vm((rows, COLS * length, kvw), BF16),
        vm((kvh, qrows, HD), BF16), vm((qrows, HD), F32),
        vm((qrows, 1), F32), vm((qrows, 1), F32),
        vm((2, length, half), F32),
        vm((8, length), F32), vm((tp - 1, 8, length), F32),
        dma((3,)), dma((3,)), dma((1,)), dma((1,)),
        dma((CHUNKS,)), dma((CHUNKS,)), dma((CHUNKS,)), dma((CHUNKS,)),
        dma((CHUNKS,)), dma((CHUNKS,)),
        dma((2, rows)), dma((2, rows)), dma((2, rows)), dma((2, rows)), dma((2, 1)),
        dma((tp - 1,)), dma((tp - 1,)),
    ]
    lift = lambda p: p.reshape(1, -1)
    spec = pl.BlockSpec(memory_space=pltpu.VMEM)
    return pl.pallas_call(
        functools.partial(kernel, n, tp, inner),
        out_shape=(
            jax.ShapeDtypeStruct(x.shape, BF16),
            jax.ShapeDtypeStruct(q.shape, BF16),
        ),
        in_specs=[spec] * 15,
        out_specs=(spec, spec),
        scratch_shapes=scratch,
        compiler_params=pltpu.CompilerParams(
            collective_id=0, has_side_effects=True, vmem_limit_bytes=60 * 1024 * 1024
        ),
    )(x, gate, b, c, step, lift(bias), lift(rate), lift(skip), cx, cb, cc, lift(gain), q, k, v)


def solution(mesh):
    n, tp = mesh.shape["seq"], mesh.shape["tp"]
    placed = (
        (P("seq", "tp"),) * 5
        + (P("tp"),) * 3
        + (P(None, "tp"),) * 3
        + (P("tp"),)
        + (P("seq", "tp"),) * 3
    )

    def run(*args):
        inner = args[0].shape[1]
        return jax.shard_map(
            functools.partial(shards, inner, n, tp),
            mesh=mesh,
            in_specs=placed,
            out_specs=(P("seq", "tp"), P("seq", "tp")),
            check_vma=False,
        )(*args)

    return run
```

```python
import functools
import math

import jax
import jax.numpy as jnp
from jax import lax
from jax.experimental import pallas as pl
from jax.experimental.pallas import tpu as pltpu
from jax.sharding import PartitionSpec as P


P_SIZE = 64
STATE = 128
HD = 128
COLS = 2
CHUNKS = 8
HALO = 16
QTILE = 256
EPS = 1e-05
LOWEST = -1e30
MESH = pl.DeviceIdType.MESH
F32 = jnp.float32
BF16 = jnp.bfloat16


def dot(a, b, ca=1, cb=0):
    return lax.dot_general(a, b, (((ca,), (cb,)), ((), ())), preferred_element_type=F32)


def pieces_of(a, terms):
    out = []
    for _ in range(terms):
        head = a.astype(BF16)
        out.append(head)
        a = a - head.astype(F32)
    return out


def silu(a):
    return a / (1.0 + jnp.exp(-a))


def kernel(
    n, tp, inner,
    x_ref, gate_ref, b_ref, c_ref, step_ref, bias_ref, rate_ref, skip_ref,
    cx_ref, cb_ref, cc_ref, gain_ref, q_ref, k_ref, v_ref,
    mix_out, att_out,
    hx, hb, hc, padx, padb, sig, scl, ex, bst, cst,
    s_buf, r1, e_in, e_out, p_out, ent, p_in, dec_own, dec_par,
    kbuf, vbuf, qs, acc, m_sc, l_sc, ybuf, sq_own, sq_in,
    halo_s, halo_r, dec_s, dec_r, p1_s, p1_r, p2_s, p2_r, p3_s, p3_r,
    kc_s, kc_r, kp_s, kp_r, kl_s, sq_s, sq_r,
):
    me = lax.axis_index("seq")
    mytp = lax.axis_index("tp")
    rows = n // COLS
    row = me // COLS
    col = me % COLS
    other = 1 - col
    partner = row * COLS + other
    length, width = x_ref.shape
    half = width // 2
    cw = half // CHUNKS
    groups = b_ref.shape[1] // STATE
    gwidth = width // groups
    heads = width // P_SIZE
    kvh = k_ref.shape[1] // HD
    qper = q_ref.shape[1] // HD // kvh

    barrier = pltpu.get_barrier_semaphore()

    @pl.loop(1, n)
    def _(d):
        pl.semaphore_signal(barrier, inc=1, device_id={"seq": (me + d) % n}, device_id_type=MESH)

    for d in range(1, tp):
        pl.semaphore_signal(
            barrier, inc=1, device_id={"tp": (mytp + d) % tp}, device_id_type=MESH
        )

    hr = lax.broadcasted_iota(jnp.int32, (heads, heads), 0)
    hc_ = lax.broadcasted_iota(jnp.int32, (heads, heads), 1)
    small = (hr == hc_).astype(F32).astype(BF16)
    turned = sum(dot(p, small, 0, 0) for p in pieces_of(step_ref[...], 3))
    pre = turned + bias_ref[...]
    dt = jnp.maximum(pre, 0.0) + jnp.log1p(jnp.exp(-jnp.abs(pre)))
    a = -dt * rate_ref[...]
    ri = lax.broadcasted_iota(jnp.int32, (length, length), 0)
    ci = lax.broadcasted_iota(jnp.int32, (length, length), 1)
    lower = (ri >= ci).astype(F32).astype(BF16)
    upper = (ri <= ci).astype(F32).astype(BF16)
    apieces = pieces_of(a, 3)
    logd = sum(dot(lower, p) for p in apieces)
    logt = sum(dot(p, upper, 0, 0) for p in apieces)
    last = logd[length - 1 : length, :]
    closing = jnp.exp(last - logd)
    hi = lax.broadcasted_iota(jnp.int32, (heads, width), 0)
    wi = lax.broadcasted_iota(jnp.int32, (heads, width), 1)
    spread = (wi // P_SIZE == hi).astype(F32).astype(BF16)
    many = jnp.concatenate([dt, dt * closing, jnp.exp(logd)], axis=0)
    wide = sum(dot(p, spread) for p in pieces_of(many, 2))
    dtx, wx, elx = wide[:length], wide[length : 2 * length], wide[2 * length :]
    skipx = sum(dot(p, spread) for p in pieces_of(jnp.broadcast_to(skip_ref[...], (8, heads)), 3))[:1]
    for h in range(2):
        cut = slice(h * half, (h + 1) * half)
        ex[h] = elx[:, cut]
        scl[h] = dtx[:, cut]
        sig[h] = wx[:, cut]
        dec_own[h] = elx[length - 1 : length, cut]

    pl.semaphore_wait(barrier, n - 1 + tp - 1)

    def halo(dst):
        out = []
        for i, (src, buf) in enumerate(((x_ref, hx), (b_ref, hb), (c_ref, hc))):
            out.append(
                pltpu.make_async_remote_copy(
                    src_ref=src.at[pl.ds(length - HALO, HALO)], dst_ref=buf,
                    send_sem=halo_s.at[i], recv_sem=halo_r.at[i],
                    device_id={"seq": dst}, device_id_type=MESH,
                )
            )
        return out

    @pl.when(me < n - 1)
    def _():
        for cp in halo(me + 1):
            cp.start()

    dec_copy = pltpu.make_async_remote_copy(
        src_ref=dec_own, dst_ref=dec_par, send_sem=dec_s.at[0], recv_sem=dec_r.at[0],
        device_id={"seq": partner}, device_id_type=MESH,
    )
    dec_copy.start()

    def place(c):
        return pl.ds(pl.multiple_of(c * length, length), length)

    def kv_copy(i, dst_row, dst_col, slot_row, slot_col, own, ss, rs, sidx, ridx):
        src = (k_ref, v_ref)[i] if own else (kbuf, vbuf)[i].at[slot_row, place(slot_col)]
        return pltpu.make_async_remote_copy(
            src_ref=src, dst_ref=(kbuf, vbuf)[i].at[slot_row, place(slot_col)],
            send_sem=ss.at[i, sidx], recv_sem=rs.at[i, ridx],
            device_id={"seq": dst_row * COLS + dst_col}, device_id_type=MESH,
        )

    def own_up(i, dst_row):
        return kv_copy(i, dst_row, col, row, col, True, kc_s, kc_r, dst_row, row)

    def own_side(i):
        return kv_copy(i, row, other, row, col, True, kl_s, kp_r, 0, row)

    def relay(i, src_row):
        return kv_copy(i, row, other, src_row, col, False, kp_s, kp_r, src_row, src_row)

    @pl.loop(row + 1, rows)
    def _(dst):
        for i in range(2):
            own_up(i, dst).start()

    kbuf[row, place(col)] = k_ref[...]
    vbuf[row, place(col)] = v_ref[...]
    for g in range(kvh):
        for h in range(qper):
            at = (g * qper + h) * HD
            qs[g, h * length : (h + 1) * length] = q_ref[:, at : at + HD]

    @pl.when(me > 0)
    def _():
        for cp in halo(me):
            cp.wait_recv()
        padx[:HALO] = hx[...].astype(F32)
        padb[0, :HALO] = hb[...].astype(F32)
        padb[1, :HALO] = hc[...].astype(F32)

    @pl.when(me == 0)
    def _():
        padx[:HALO] = jnp.zeros((HALO, width), F32)
        padb[:, :HALO] = jnp.zeros((2, HALO, b_ref.shape[1]), F32)

    padx[HALO:] = x_ref[...].astype(F32)
    padb[0, HALO:] = b_ref[...].astype(F32)
    padb[1, HALO:] = c_ref[...].astype(F32)
    taps = cx_ref.shape[0]

    def conv(load, w_ref, cut):
        total = None
        for k in range(taps):
            at = HALO - (taps - 1) + k
            term = w_ref[k : k + 1, cut] * load(at)
            total = term if total is None else total + term
        return silu(total)

    for g in range(groups):
        cut = slice(g * STATE, (g + 1) * STATE)
        bst[g] = conv(lambda at: padb[0, at : at + length, cut], cb_ref, cut).astype(BF16)
        cst[g] = conv(lambda at: padb[1, at : at + length, cut], cc_ref, cut).astype(BF16)
    def group_of(h, j):
        return h * (groups // 2) + (j * cw) // gwidth

    def p1(j):
        return pltpu.make_async_remote_copy(
            src_ref=s_buf.at[other, j], dst_ref=r1.at[j],
            send_sem=p1_s.at[j], recv_sem=p1_r.at[j],
            device_id={"seq": partner}, device_id_type=MESH,
        )

    def local_state(h, j):
        loc = slice(j * cw, (j + 1) * cw)
        cut = pl.ds(pl.multiple_of(h * half + j * cw, 128), cw)
        u = conv(lambda at: padx[at : at + length, cut], cx_ref, cut)
        weighted = (u * sig[h, :, loc]).astype(BF16)
        sig[h, :, loc] = u
        scl[h, :, loc] = u * scl[h, :, loc]
        s_buf[h, j] = dot(bst[group_of(h, j)], weighted, 0, 0).astype(BF16)

    for j in range(CHUNKS):
        local_state(other, j)
        p1(j).start()
    for i in range(2):
        own_side(i).start()
    for j in range(CHUNKS):
        local_state(col, j)

    @pl.loop(0, row)
    def _(src):
        for i in range(2):
            own = kv_copy(i, row, col, src, col, False, kc_s, kc_r, row, src)
            own.wait_recv()
            relay(i, src).start()

    causal = ri >= ci
    lane = lax.broadcasted_iota(jnp.int32, (length, 128), 1)
    per = 128 // P_SIZE
    for g in range(groups):
        coup = dot(cst[g], bst[g], 1, 1)
        coup = jnp.where(causal, coup, 0.0)
        for t in range(gwidth // 128):
            at = g * gwidth + t * 128
            h, loc = at // half, at % half
            tile = scl[h, :, loc : loc + 128].astype(BF16)
            res = None
            for p in range(per):
                hd = at // P_SIZE + p
                diff = logd[:, hd : hd + 1] - logt[hd : hd + 1, :]
                mixing = (jnp.exp(jnp.minimum(diff, 0.0)) * coup).astype(BF16)
                y = dot(mixing, tile)
                res = y if res is None else jnp.where(lane >= p * P_SIZE, y, res)
            ybuf[h, :, loc : loc + 128] = res + skipx[:, at : at + 128] * sig[h, :, loc : loc + 128]

    scale = math.log2(math.e) / math.sqrt(HD)
    qrows = qper * length
    eye = (ri == ci).astype(F32).astype(BF16)

    def attend(lo, hi):
        @pl.loop(lo, hi)
        def _(g):
            m_sc[...] = jnp.full((1, qrows), LOWEST, F32)
            l_sc[...] = jnp.zeros((1, qrows), F32)
            acc[...] = jnp.zeros((HD, qrows), F32)
            lanes = pl.ds(pl.multiple_of(g * HD, HD), HD)

            def step(r, masked):
                keys = kbuf[r, :, lanes]
                vals = vbuf[r, :, lanes].T
                for t in range(qrows // QTILE):
                    cut = slice(t * QTILE, (t + 1) * QTILE)
                    s = dot(keys, qs[g, cut], 1, 1) * scale
                    if masked:
                        ki = lax.broadcasted_iota(jnp.int32, s.shape, 0)
                        qi = lax.broadcasted_iota(jnp.int32, s.shape, 1) % length + col * length
                        s = jnp.where(ki <= qi, s, LOWEST)
                    old = m_sc[:, cut]
                    new = jnp.maximum(old, jnp.max(s, axis=0, keepdims=True))
                    p = jnp.exp2(s - new)
                    f = jnp.exp2(old - new)
                    m_sc[:, cut] = new
                    l_sc[:, cut] = l_sc[:, cut] * f + jnp.sum(p, axis=0, keepdims=True)
                    acc[:, cut] = acc[:, cut] * f + dot(vals, p.astype(BF16))

            step(row, True)

            @pl.loop(0, row)
            def _(r):
                step(r, False)

            for h in range(qper):
                cut = slice(h * length, (h + 1) * length)
                out = (acc[:, cut] / l_sc[:, cut]).astype(BF16)
                at = pl.multiple_of((g * qper + h) * HD, HD)
                att_out[:, pl.ds(at, HD)] = dot(eye, out, 1, 1).astype(BF16)

    @pl.loop(0, row)
    def _(src):
        for i in range(2):
            relay(i, src).wait_recv()

    for i in range(2):
        own_side(i).wait_recv()
    early = jnp.where(row == rows - 1, kvh, 0)
    attend(0, early)

    dec_copy.wait_recv()

    def p2(j, dst_row):
        return pltpu.make_async_remote_copy(
            src_ref=e_out.at[j], dst_ref=e_in.at[j],
            send_sem=p2_s.at[j], recv_sem=p2_r.at[j],
            device_id={"seq": dst_row * COLS + col}, device_id_type=MESH,
        )

    def p3(j):
        return pltpu.make_async_remote_copy(
            src_ref=p_out.at[j], dst_ref=p_in.at[j],
            send_sem=p3_s.at[j], recv_sem=p3_r.at[j],
            device_id={"seq": partner}, device_id_type=MESH,
        )

    @pl.when(row == 0)
    def _():
        e_in[...] = jnp.zeros(e_in.shape, BF16)

    first_col = col == 0
    for j in range(CHUNKS):
        loc = slice(j * cw, (j + 1) * cw)
        do, dp = dec_own[col, :, loc], dec_par[col, :, loc]
        p1(j).wait_recv()

        @pl.when(row > 0)
        def _():
            p2(j, row).wait_recv()

        so = s_buf[col, j].astype(F32)
        sr = r1[j].astype(F32)
        e = e_in[j].astype(F32)
        earlier = jnp.where(first_col, so, sr)
        later = jnp.where(first_col, sr, so)
        dec_a = jnp.where(first_col, do, dp)
        dec_b = jnp.where(first_col, dp, do)
        mid = dec_a * e + earlier

        @pl.when(row < rows - 1)
        def _():
            e_out[j] = (dec_b * mid + later).astype(BF16)
            p2(j, row + 1).start()

        p_out[j] = jnp.where(first_col, mid, e).astype(BF16)
        p3(j).start()
        ent[j] = jnp.where(first_col, e, mid).astype(BF16)

    attend(early, kvh)

    ones = jnp.ones((8, cw), F32).astype(BF16)
    sums = jnp.zeros((8, length), F32)

    def close(h, j, state):
        loc = slice(j * cw, (j + 1) * cw)
        y = ybuf[h, :, loc] + ex[h, :, loc] * dot(cst[group_of(h, j)], state)
        at = pl.ds(pl.multiple_of(h * half + j * cw, cw), cw)
        y = y * silu(gate_ref[:, at].astype(F32))
        ybuf[h, :, loc] = y
        return y * y

    squares = None
    for j in range(CHUNKS):
        s = close(col, j, ent[j])
        squares = s if squares is None else squares + s
    for j in range(CHUNKS):
        p3(j).wait_recv()
        squares = squares + close(other, j, p_in[j])
    for p in pieces_of(squares, 3):
        sums = sums + dot(ones, p, 1, 1)
    sq_own[...] = sums

    def sq(d):
        return pltpu.make_async_remote_copy(
            src_ref=sq_own, dst_ref=sq_in.at[d - 1],
            send_sem=sq_s.at[d - 1], recv_sem=sq_r.at[d - 1],
            device_id={"tp": (mytp + d) % tp}, device_id_type=MESH,
        )

    for d in range(1, tp):
        sq(d).start()
    for d in range(1, tp):
        sq(d).wait_recv()
        sums = sums + sq_in[d - 1]
    scal = lax.rsqrt(sums / inner + EPS)
    eighth = jnp.full((8, 128), 0.125, F32).astype(BF16)
    column = sum(dot(p, eighth, 0, 0) for p in pieces_of(scal, 3))
    for t in range(width // 128):
        h, loc = (t * 128) // half, (t * 128) % half
        cut = slice(t * 128, (t + 1) * 128)
        mix_out[:, cut] = (ybuf[h, :, loc : loc + 128] * column * gain_ref[:, cut]).astype(BF16)

    for d in range(1, tp):
        sq(d).wait_send()
    for j in range(CHUNKS):
        p1(j).wait_send()
        p3(j).wait_send()
    dec_copy.wait_send()
    for i in range(2):
        own_side(i).wait_send()

    @pl.when(row < rows - 1)
    def _():
        for j in range(CHUNKS):
            p2(j, row + 1).wait_send()

    @pl.when(me < n - 1)
    def _():
        for cp in halo(me + 1):
            cp.wait_send()

    @pl.loop(row + 1, rows)
    def _(dst):
        for i in range(2):
            own_up(i, dst).wait_send()

    @pl.loop(0, row)
    def _(src):
        for i in range(2):
            relay(i, src).wait_send()


def shards(inner, n, tp, x, gate, b, c, step, bias, rate, skip, cx, cb, cc, gain, q, k, v):
    length, width = x.shape
    half = width // 2
    cw = half // CHUNKS
    groups = b.shape[1] // STATE
    kvw = k.shape[1]
    kvh = kvw // HD
    qrows = q.shape[1] // HD // kvh * length
    rows = n // COLS
    vm, dma = pltpu.VMEM, pltpu.SemaphoreType.DMA
    chunk = (CHUNKS, STATE, cw)
    scratch = [
        vm((HALO, width), BF16), vm((HALO, b.shape[1]), BF16), vm((HALO, b.shape[1]), BF16),
        vm((HALO + length, width), F32), vm((2, HALO + length, b.shape[1]), F32),
        vm((2, length, half), F32),
        vm((2, length, half), F32), vm((2, length, half), F32),
        vm((groups, length, STATE), BF16), vm((groups, length, STATE), BF16),
        vm((2,) + chunk, BF16), vm(chunk, BF16), vm(chunk, BF16), vm(chunk, BF16),
        vm(chunk, BF16), vm(chunk, BF16), vm(chunk, BF16),
        vm((2, 1, half), F32), vm((2, 1, half), F32),
        vm((rows, COLS * length, kvw), BF16), vm((rows, COLS * length, kvw), BF16),
        vm((kvh, qrows, HD), BF16), vm((HD, qrows), F32),
        vm((1, qrows), F32), vm((1, qrows), F32),
        vm((2, length, half), F32),
        vm((8, length), F32), vm((tp - 1, 8, length), F32),
        dma((3,)), dma((3,)), dma((1,)), dma((1,)),
        dma((CHUNKS,)), dma((CHUNKS,)), dma((CHUNKS,)), dma((CHUNKS,)),
        dma((CHUNKS,)), dma((CHUNKS,)),
        dma((2, rows)), dma((2, rows)), dma((2, rows)), dma((2, rows)), dma((2, 1)),
        dma((tp - 1,)), dma((tp - 1,)),
    ]
    lift = lambda p: p.reshape(1, -1)
    spec = pl.BlockSpec(memory_space=pltpu.VMEM)
    return pl.pallas_call(
        functools.partial(kernel, n, tp, inner),
        out_shape=(
            jax.ShapeDtypeStruct(x.shape, BF16),
            jax.ShapeDtypeStruct(q.shape, BF16),
        ),
        in_specs=[spec] * 15,
        out_specs=(spec, spec),
        scratch_shapes=scratch,
        compiler_params=pltpu.CompilerParams(
            collective_id=0, has_side_effects=True, vmem_limit_bytes=60 * 1024 * 1024
        ),
    )(x, gate, b, c, step.T, lift(bias), lift(rate), lift(skip), cx, cb, cc, lift(gain), q, k, v)


def solution(mesh):
    n, tp = mesh.shape["seq"], mesh.shape["tp"]
    placed = (
        (P("seq", "tp"),) * 5
        + (P("tp"),) * 3
        + (P(None, "tp"),) * 3
        + (P("tp"),)
        + (P("seq", "tp"),) * 3
    )

    def run(*args):
        inner = args[0].shape[1]
        return jax.shard_map(
            functools.partial(shards, inner, n, tp),
            mesh=mesh,
            in_specs=placed,
            out_specs=(P("seq", "tp"), P("seq", "tp")),
            check_vma=False,
        )(*args)

    return run
```

```python
import functools
import math

import jax
import jax.numpy as jnp
from jax import lax
from jax.experimental import pallas as pl
from jax.experimental.pallas import tpu as pltpu
from jax.sharding import PartitionSpec as P


P_SIZE = 64
STATE = 128
HD = 128
COLS = 2
CHUNKS = 8
HALO = 16
QTILE = 256
EPS = 1e-05
LOWEST = -1e30
MESH = pl.DeviceIdType.MESH
F32 = jnp.float32
BF16 = jnp.bfloat16


def dot(a, b, ca=1, cb=0):
    return lax.dot_general(a, b, (((ca,), (cb,)), ((), ())), preferred_element_type=F32)


def pieces_of(a, terms):
    out = []
    for _ in range(terms):
        head = a.astype(BF16)
        out.append(head)
        a = a - head.astype(F32)
    return out


def silu(a):
    return a / (1.0 + jnp.exp(-a))


def kernel(
    n, tp, inner,
    x_ref, gate_ref, b_ref, c_ref, step_ref, bias_ref, rate_ref, skip_ref,
    cx_ref, cb_ref, cc_ref, gain_ref, q_ref, k_ref, v_ref,
    mix_out, att_out,
    hx, hb, hc, padx, padb, sig, scl, ex, bst, cst,
    s_buf, r1, e_in, e_out, p_out, ent, p_in, dec_own, dec_par,
    kbuf, vbuf, qs, acc, m_sc, l_sc, ybuf, sq_own, sq_in,
    halo_s, halo_r, dec_s, dec_r, p1_s, p1_r, p2_s, p2_r, p3_s, p3_r,
    kc_s, kc_r, kp_s, kp_r, kl_s, sq_s, sq_r,
):
    me = lax.axis_index("seq")
    mytp = lax.axis_index("tp")
    rows = n // COLS
    row = me // COLS
    col = me % COLS
    other = 1 - col
    partner = row * COLS + other
    length, width = x_ref.shape
    half = width // 2
    cw = half // CHUNKS
    groups = b_ref.shape[1] // STATE
    gwidth = width // groups
    heads = width // P_SIZE
    kvh = k_ref.shape[1] // HD
    qper = q_ref.shape[1] // HD // kvh

    barrier = pltpu.get_barrier_semaphore()

    @pl.loop(1, n)
    def _(d):
        pl.semaphore_signal(barrier, inc=1, device_id={"seq": (me + d) % n}, device_id_type=MESH)

    for d in range(1, tp):
        pl.semaphore_signal(
            barrier, inc=1, device_id={"tp": (mytp + d) % tp}, device_id_type=MESH
        )

    hr = lax.broadcasted_iota(jnp.int32, (heads, heads), 0)
    hc_ = lax.broadcasted_iota(jnp.int32, (heads, heads), 1)
    small = (hr == hc_).astype(F32).astype(BF16)
    turned = sum(dot(p, small, 0, 0) for p in pieces_of(step_ref[...], 3))
    pre = turned + bias_ref[...]
    dt = jnp.maximum(pre, 0.0) + jnp.log1p(jnp.exp(-jnp.abs(pre)))
    a = -dt * rate_ref[...]
    ri = lax.broadcasted_iota(jnp.int32, (length, length), 0)
    ci = lax.broadcasted_iota(jnp.int32, (length, length), 1)
    lower = (ri >= ci).astype(F32).astype(BF16)
    upper = (ri <= ci).astype(F32).astype(BF16)
    apieces = pieces_of(a, 3)
    logd = sum(dot(lower, p) for p in apieces)
    logt = sum(dot(p, upper, 0, 0) for p in apieces)
    last = logd[length - 1 : length, :]
    closing = jnp.exp(last - logd)
    hi = lax.broadcasted_iota(jnp.int32, (heads, width), 0)
    wi = lax.broadcasted_iota(jnp.int32, (heads, width), 1)
    spread = (wi // P_SIZE == hi).astype(F32).astype(BF16)
    many = jnp.concatenate([dt, dt * closing, jnp.exp(logd)], axis=0)
    wide = sum(dot(p, spread) for p in pieces_of(many, 2))
    dtx, wx, elx = wide[:length], wide[length : 2 * length], wide[2 * length :]
    skipx = sum(dot(p, spread) for p in pieces_of(jnp.broadcast_to(skip_ref[...], (8, heads)), 3))[:1]
    for h in range(2):
        cut = slice(h * half, (h + 1) * half)
        ex[h] = elx[:, cut]
        scl[h] = dtx[:, cut]
        sig[h] = wx[:, cut]
        dec_own[h] = elx[length - 1 : length, cut]

    pl.semaphore_wait(barrier, n - 1 + tp - 1)

    def halo(dst):
        out = []
        for i, (src, buf) in enumerate(((x_ref, hx), (b_ref, hb), (c_ref, hc))):
            out.append(
                pltpu.make_async_remote_copy(
                    src_ref=src.at[pl.ds(length - HALO, HALO)], dst_ref=buf,
                    send_sem=halo_s.at[i], recv_sem=halo_r.at[i],
                    device_id={"seq": dst}, device_id_type=MESH,
                )
            )
        return out

    @pl.when(me < n - 1)
    def _():
        for cp in halo(me + 1):
            cp.start()

    dec_copy = pltpu.make_async_remote_copy(
        src_ref=dec_own, dst_ref=dec_par, send_sem=dec_s.at[0], recv_sem=dec_r.at[0],
        device_id={"seq": partner}, device_id_type=MESH,
    )
    dec_copy.start()

    def place(c):
        return pl.ds(pl.multiple_of(c * length, length), length)

    def kv_copy(i, dst_row, dst_col, slot_row, slot_col, own, ss, rs, sidx, ridx):
        src = (k_ref, v_ref)[i] if own else (kbuf, vbuf)[i].at[slot_row, place(slot_col)]
        return pltpu.make_async_remote_copy(
            src_ref=src, dst_ref=(kbuf, vbuf)[i].at[slot_row, place(slot_col)],
            send_sem=ss.at[i, sidx], recv_sem=rs.at[i, ridx],
            device_id={"seq": dst_row * COLS + dst_col}, device_id_type=MESH,
        )

    def own_up(i, dst_row):
        return kv_copy(i, dst_row, col, row, col, True, kc_s, kc_r, dst_row, row)

    def own_side(i):
        return kv_copy(i, row, other, row, col, True, kl_s, kp_r, 0, row)

    def relay(i, src_row):
        return kv_copy(i, row, other, src_row, col, False, kp_s, kp_r, src_row, src_row)

    @pl.loop(row + 1, rows)
    def _(dst):
        for i in range(2):
            own_up(i, dst).start()

    kbuf[row, place(col)] = k_ref[...]
    vbuf[row, place(col)] = v_ref[...]
    for g in range(kvh):
        for h in range(qper):
            at = (g * qper + h) * HD
            qs[g, h * length : (h + 1) * length] = q_ref[:, at : at + HD]

    @pl.when(me > 0)
    def _():
        for cp in halo(me):
            cp.wait_recv()
        padx[:HALO] = hx[...].astype(F32)
        padb[0, :HALO] = hb[...].astype(F32)
        padb[1, :HALO] = hc[...].astype(F32)

    @pl.when(me == 0)
    def _():
        padx[:HALO] = jnp.zeros((HALO, width), F32)
        padb[:, :HALO] = jnp.zeros((2, HALO, b_ref.shape[1]), F32)

    def pass_on(lo, hi):
        @pl.loop(lo, hi)
        def _(at):
            src = row - 1 - at
            for i in range(2):
                kv_copy(i, row, col, src, col, False, kc_s, kc_r, row, src).wait_recv()
                relay(i, src).start()

    final_row = row == rows - 1

    padx[HALO:] = x_ref[...].astype(F32)
    padb[0, HALO:] = b_ref[...].astype(F32)
    padb[1, HALO:] = c_ref[...].astype(F32)
    taps = cx_ref.shape[0]

    def conv(load, w_ref, cut):
        total = None
        for k in range(taps):
            at = HALO - (taps - 1) + k
            term = w_ref[k : k + 1, cut] * load(at)
            total = term if total is None else total + term
        return silu(total)

    for g in range(groups):
        cut = slice(g * STATE, (g + 1) * STATE)
        bst[g] = conv(lambda at: padb[0, at : at + length, cut], cb_ref, cut).astype(BF16)
        cst[g] = conv(lambda at: padb[1, at : at + length, cut], cc_ref, cut).astype(BF16)
    def group_of(h, j):
        return h * (groups // 2) + (j * cw) // gwidth

    def p1(j):
        return pltpu.make_async_remote_copy(
            src_ref=s_buf.at[other, j], dst_ref=r1.at[j],
            send_sem=p1_s.at[j], recv_sem=p1_r.at[j],
            device_id={"seq": partner}, device_id_type=MESH,
        )

    def local_state(h, j):
        loc = slice(j * cw, (j + 1) * cw)
        cut = pl.ds(pl.multiple_of(h * half + j * cw, 128), cw)
        u = conv(lambda at: padx[at : at + length, cut], cx_ref, cut)
        weighted = (u * sig[h, :, loc]).astype(BF16)
        sig[h, :, loc] = u
        scl[h, :, loc] = u * scl[h, :, loc]
        s_buf[h, j] = dot(bst[group_of(h, j)], weighted, 0, 0).astype(BF16)

    for j in range(CHUNKS):
        local_state(other, j)
        p1(j).start()
    for i in range(2):
        own_side(i).start()
    for j in range(CHUNKS):
        local_state(col, j)

    causal = ri >= ci
    lane = lax.broadcasted_iota(jnp.int32, (length, 128), 1)
    per = 128 // P_SIZE
    for g in range(groups):
        coup = dot(cst[g], bst[g], 1, 1)
        coup = jnp.where(causal, coup, 0.0)
        for t in range(gwidth // 128):
            at = g * gwidth + t * 128
            h, loc = at // half, at % half
            tile = scl[h, :, loc : loc + 128].astype(BF16)
            res = None
            for p in range(per):
                hd = at // P_SIZE + p
                diff = logd[:, hd : hd + 1] - logt[hd : hd + 1, :]
                mixing = (jnp.exp(jnp.minimum(diff, 0.0)) * coup).astype(BF16)
                y = dot(mixing, tile)
                res = y if res is None else jnp.where(lane >= p * P_SIZE, y, res)
            ybuf[h, :, loc : loc + 128] = res + skipx[:, at : at + 128] * sig[h, :, loc : loc + 128]

    pass_on(0, row)
    scale = math.log2(math.e) / math.sqrt(HD)
    qrows = qper * length
    eye = (ri == ci).astype(F32).astype(BF16)

    def attend(lo, hi):
        @pl.loop(lo, hi)
        def _(g):
            m_sc[...] = jnp.full((1, qrows), LOWEST, F32)
            l_sc[...] = jnp.zeros((1, qrows), F32)
            acc[...] = jnp.zeros((HD, qrows), F32)
            lanes = pl.ds(pl.multiple_of(g * HD, HD), HD)

            def step(r, masked):
                keys = kbuf[r, :, lanes]
                vals = vbuf[r, :, lanes].T
                for t in range(qrows // QTILE):
                    cut = slice(t * QTILE, (t + 1) * QTILE)
                    s = dot(keys, qs[g, cut], 1, 1) * scale
                    if masked:
                        ki = lax.broadcasted_iota(jnp.int32, s.shape, 0)
                        qi = lax.broadcasted_iota(jnp.int32, s.shape, 1) % length + col * length
                        s = jnp.where(ki <= qi, s, LOWEST)
                    old = m_sc[:, cut]
                    new = jnp.maximum(old, jnp.max(s, axis=0, keepdims=True))
                    p = jnp.exp2(s - new)
                    f = jnp.exp2(old - new)
                    m_sc[:, cut] = new
                    l_sc[:, cut] = l_sc[:, cut] * f + jnp.sum(p, axis=0, keepdims=True)
                    acc[:, cut] = acc[:, cut] * f + dot(vals, p.astype(BF16))

            step(row, True)

            @pl.loop(0, row)
            def _(r):
                step(r, False)

            for h in range(qper):
                cut = slice(h * length, (h + 1) * length)
                out = (acc[:, cut] / l_sc[:, cut]).astype(BF16)
                at = pl.multiple_of((g * qper + h) * HD, HD)
                att_out[:, pl.ds(at, HD)] = dot(eye, out, 1, 1).astype(BF16)

    def gathered(lo, hi):
        @pl.loop(lo, hi)
        def _(src):
            for i in range(2):
                relay(i, src).wait_recv()

    early = jnp.where(final_row, kvh // 2, 0)
    soon = jnp.where(final_row, row, 0)
    gathered(0, soon)
    for i in range(2):
        own_side(i).wait_recv()
    attend(0, early)

    dec_copy.wait_recv()

    def p2(j, dst_row):
        return pltpu.make_async_remote_copy(
            src_ref=e_out.at[j], dst_ref=e_in.at[j],
            send_sem=p2_s.at[j], recv_sem=p2_r.at[j],
            device_id={"seq": dst_row * COLS + col}, device_id_type=MESH,
        )

    def p3(j):
        return pltpu.make_async_remote_copy(
            src_ref=p_out.at[j], dst_ref=p_in.at[j],
            send_sem=p3_s.at[j], recv_sem=p3_r.at[j],
            device_id={"seq": partner}, device_id_type=MESH,
        )

    @pl.when(row == 0)
    def _():
        e_in[...] = jnp.zeros(e_in.shape, BF16)

    first_col = col == 0
    for j in range(CHUNKS):
        loc = slice(j * cw, (j + 1) * cw)
        do, dp = dec_own[col, :, loc], dec_par[col, :, loc]
        p1(j).wait_recv()

        @pl.when(row > 0)
        def _():
            p2(j, row).wait_recv()

        so = s_buf[col, j].astype(F32)
        sr = r1[j].astype(F32)
        e = e_in[j].astype(F32)
        earlier = jnp.where(first_col, so, sr)
        later = jnp.where(first_col, sr, so)
        dec_a = jnp.where(first_col, do, dp)
        dec_b = jnp.where(first_col, dp, do)
        mid = dec_a * e + earlier

        @pl.when(row < rows - 1)
        def _():
            e_out[j] = (dec_b * mid + later).astype(BF16)
            p2(j, row + 1).start()

        p_out[j] = jnp.where(first_col, mid, e).astype(BF16)
        p3(j).start()
        ent[j] = jnp.where(first_col, e, mid).astype(BF16)

    gathered(soon, row)
    attend(early, kvh)

    ones = jnp.ones((8, cw), F32).astype(BF16)
    sums = jnp.zeros((8, length), F32)

    def close(h, j, state):
        loc = slice(j * cw, (j + 1) * cw)
        y = ybuf[h, :, loc] + ex[h, :, loc] * dot(cst[group_of(h, j)], state)
        at = pl.ds(pl.multiple_of(h * half + j * cw, cw), cw)
        y = y * silu(gate_ref[:, at].astype(F32))
        ybuf[h, :, loc] = y
        return y * y

    squares = None
    for j in range(CHUNKS):
        s = close(col, j, ent[j])
        squares = s if squares is None else squares + s
    for j in range(CHUNKS):
        p3(j).wait_recv()
        squares = squares + close(other, j, p_in[j])
    for p in pieces_of(squares, 3):
        sums = sums + dot(ones, p, 1, 1)
    sq_own[...] = sums

    def sq(d):
        return pltpu.make_async_remote_copy(
            src_ref=sq_own, dst_ref=sq_in.at[d - 1],
            send_sem=sq_s.at[d - 1], recv_sem=sq_r.at[d - 1],
            device_id={"tp": (mytp + d) % tp}, device_id_type=MESH,
        )

    for d in range(1, tp):
        sq(d).start()
    for d in range(1, tp):
        sq(d).wait_recv()
        sums = sums + sq_in[d - 1]
    scal = lax.rsqrt(sums / inner + EPS)
    eighth = jnp.full((8, 128), 0.125, F32).astype(BF16)
    column = sum(dot(p, eighth, 0, 0) for p in pieces_of(scal, 3))
    for t in range(width // 128):
        h, loc = (t * 128) // half, (t * 128) % half
        cut = slice(t * 128, (t + 1) * 128)
        mix_out[:, cut] = (ybuf[h, :, loc : loc + 128] * column * gain_ref[:, cut]).astype(BF16)

    for d in range(1, tp):
        sq(d).wait_send()
    for j in range(CHUNKS):
        p1(j).wait_send()
        p3(j).wait_send()
    dec_copy.wait_send()
    for i in range(2):
        own_side(i).wait_send()

    @pl.when(row < rows - 1)
    def _():
        for j in range(CHUNKS):
            p2(j, row + 1).wait_send()

    @pl.when(me < n - 1)
    def _():
        for cp in halo(me + 1):
            cp.wait_send()

    @pl.loop(row + 1, rows)
    def _(dst):
        for i in range(2):
            own_up(i, dst).wait_send()

    @pl.loop(0, row)
    def _(src):
        for i in range(2):
            relay(i, src).wait_send()


def shards(inner, n, tp, x, gate, b, c, step, bias, rate, skip, cx, cb, cc, gain, q, k, v):
    length, width = x.shape
    half = width // 2
    cw = half // CHUNKS
    groups = b.shape[1] // STATE
    kvw = k.shape[1]
    kvh = kvw // HD
    qrows = q.shape[1] // HD // kvh * length
    rows = n // COLS
    vm, dma = pltpu.VMEM, pltpu.SemaphoreType.DMA
    chunk = (CHUNKS, STATE, cw)
    scratch = [
        vm((HALO, width), BF16), vm((HALO, b.shape[1]), BF16), vm((HALO, b.shape[1]), BF16),
        vm((HALO + length, width), F32), vm((2, HALO + length, b.shape[1]), F32),
        vm((2, length, half), F32),
        vm((2, length, half), F32), vm((2, length, half), F32),
        vm((groups, length, STATE), BF16), vm((groups, length, STATE), BF16),
        vm((2,) + chunk, BF16), vm(chunk, BF16), vm(chunk, BF16), vm(chunk, BF16),
        vm(chunk, BF16), vm(chunk, BF16), vm(chunk, BF16),
        vm((2, 1, half), F32), vm((2, 1, half), F32),
        vm((rows, COLS * length, kvw), BF16), vm((rows, COLS * length, kvw), BF16),
        vm((kvh, qrows, HD), BF16), vm((HD, qrows), F32),
        vm((1, qrows), F32), vm((1, qrows), F32),
        vm((2, length, half), F32),
        vm((8, length), F32), vm((tp - 1, 8, length), F32),
        dma((3,)), dma((3,)), dma((1,)), dma((1,)),
        dma((CHUNKS,)), dma((CHUNKS,)), dma((CHUNKS,)), dma((CHUNKS,)),
        dma((CHUNKS,)), dma((CHUNKS,)),
        dma((2, rows)), dma((2, rows)), dma((2, rows)), dma((2, rows)), dma((2, 1)),
        dma((tp - 1,)), dma((tp - 1,)),
    ]
    lift = lambda p: p.reshape(1, -1)
    spec = pl.BlockSpec(memory_space=pltpu.VMEM)
    return pl.pallas_call(
        functools.partial(kernel, n, tp, inner),
        out_shape=(
            jax.ShapeDtypeStruct(x.shape, BF16),
            jax.ShapeDtypeStruct(q.shape, BF16),
        ),
        in_specs=[spec] * 15,
        out_specs=(spec, spec),
        scratch_shapes=scratch,
        compiler_params=pltpu.CompilerParams(
            collective_id=0, has_side_effects=True, vmem_limit_bytes=60 * 1024 * 1024
        ),
    )(x, gate, b, c, step.T, lift(bias), lift(rate), lift(skip), cx, cb, cc, lift(gain), q, k, v)


def solution(mesh):
    n, tp = mesh.shape["seq"], mesh.shape["tp"]
    placed = (
        (P("seq", "tp"),) * 5
        + (P("tp"),) * 3
        + (P(None, "tp"),) * 3
        + (P("tp"),)
        + (P("seq", "tp"),) * 3
    )

    def run(*args):
        inner = args[0].shape[1]
        return jax.shard_map(
            functools.partial(shards, inner, n, tp),
            mesh=mesh,
            in_specs=placed,
            out_specs=(P("seq", "tp"), P("seq", "tp")),
            check_vma=False,
        )(*args)

    return run
```
